32 devices in a mesh: lat: 8 (over y, x, core), lon: 4 (over z).
Axes of the slice: x: 2, y: 2, z: 4, core: 2. Of those that a mesh axis runs over, the one named last changes fastest.
Arguments:
- coeffs_old: float32 [640, 2, 3, 50, 640], P(('lat', 'lon')), may hold values from -0.16 to 0.16
- noise: bfloat16 [640, 2, 3, 50, 640], P(('lat', 'lon')), may hold values from -6 to 6
- legendre: float32 [640, 640, 640], P(('lat', 'lon')), may hold values from -0.25 to 0.25
- decay: float32 [3], replicated, may hold values from 0.3 to 0.97
- amplitude: float32 [3, 640], replicated, may hold values from 0.005 to 0.05
- wavenumber_of_slot: int32 [640], replicated, may hold values from 0 to 639, as said below
- lat_order: int32 [640], replicated, may hold values from 0 to 639, each once
Outputs:
- coeffs_new: float32 [640, 2, 3, 50, 640], P(('lat', 'lon'))
- pattern: float32 [640, 50, 1280], P(('lat', 'lon'))
The draws below stay inside these ranges and needn't reach their ends.
Inputs may be any that keep to these rules, and one draw needn't show every extreme that they name: `wavenumber_of_slot`: every wavenumber fills exactly one slot; the sums of the wavenumbers of one device's 20 slots differ between devices by less than 32. `lat_order`: every latitude stands in exactly one row.
All inputs are finite; a program needn't handle non-finite values.
Results may differ from the reference program's by a relative error of at most 0.0003.
Values sent between devices are 32-bit elements; how exact they have to be, the bound alone decides.
A program may use at most 192 MiB of HBM per device.

```python
import math
import jax
import jax.numpy as jnp
from jax import lax

M = 640
LAT = 640
LON = 1280
SCALES = 3
MEMBERS = 50
SLOT_DEV = 20


def draw_wavenumber_of_slot(key, part):
    devices_all = M // SLOT_DEV
    position = jax.random.permutation(jax.random.fold_in(key, 11), devices_all).astype(jnp.int32)
    rounds = jnp.arange(SLOT_DEV, dtype=jnp.int32)
    dealt = jnp.where(rounds[None, :] % 2 == 0, position[:, None], devices_all - 1 - position[:, None])
    table = rounds[None, :] * devices_all + dealt
    return table.reshape(-1).astype(jnp.int32)


def shard_levels(stream_key, shape, cuts, low, high):
    def one(dim, blocks):
        steps = jax.random.uniform(jax.random.fold_in(jax.random.fold_in(stream_key, 6), dim), (blocks,), jnp.float32, low / len(cuts), high / len(cuts))
        return jnp.repeat(jnp.exp(steps), shape[dim] // blocks).reshape((-1,) + (1,) * (len(shape) - dim - 1))

    loudness = one(*cuts[0])
    for cut in cuts[1:]:
        loudness = loudness * one(*cut)
    return loudness


def scatter_about(own_key, dims, scale, bound, shards=(), kind=jnp.bfloat16):
    result = scale * jax.random.normal(own_key, dims, jnp.float32)
    if shards:
        result = result * shard_levels(own_key, dims, shards, -0.22, 0.18)
    return jnp.clip(result, -bound, bound).astype(kind)


def setup_inputs(seed: int = 0) -> dict:
    arg_keys = jax.random.split(jax.random.key(seed), 8)
    coeffs_old = scatter_about(arg_keys[0], (M, 2, SCALES, MEMBERS, M), 0.02, 0.16, ((0, 32),), jnp.float32)
    noise = scatter_about(arg_keys[1], (M, 2, SCALES, MEMBERS, M), 1.0, 6.0, ((0, 32),))
    legendre = scatter_about(arg_keys[2], (M, LAT, M), M ** -0.5, 0.25, ((0, 32),), jnp.float32)
    decay = jnp.clip(jax.random.uniform(arg_keys[3], (SCALES,), jnp.float32, 0.3, 0.97), 0.3, 0.97)
    amplitude = jnp.clip(jnp.exp(jax.random.uniform(arg_keys[4], (SCALES, M), jnp.float32, math.log(0.005), math.log(0.05))), 0.005, 0.05)
    wavenumber_of_slot = draw_wavenumber_of_slot(jax.random.fold_in(arg_keys[7], 71), 0)
    lat_order = jax.random.permutation(arg_keys[6], LAT).astype(jnp.int32)
    return {"coeffs_old": coeffs_old, "noise": noise, "legendre": legendre, "decay": decay, "amplitude": amplitude, "wavenumber_of_slot": wavenumber_of_slot, "lat_order": lat_order}


def evolve(coeffs_old, noise, decay, amplitude, waves):
    width = coeffs_old.shape[4]
    offsets = lax.broadcasted_iota(jnp.int32, (waves.shape[0], width), 1)
    live = waves[:, None] + offsets < width
    padded = jnp.concatenate([amplitude, jnp.zeros_like(amplitude)], axis=1)
    spread = jax.vmap(lambda wave: lax.dynamic_slice_in_dim(padded, wave, width, 1))(waves)
    factor = jnp.sqrt(1.0 - decay * decay)
    fresh = decay[None, None, :, None, None] * coeffs_old + (spread * factor[None, :, None])[:, None, :, None, :] * noise.astype(jnp.float32)
    return jnp.where(live[:, None, None, None, :], fresh, jnp.zeros_like(fresh))

def reference(coeffs_old, noise, legendre, decay, amplitude, wavenumber_of_slot, lat_order):
    waves = wavenumber_of_slot.astype(jnp.int32)
    coeffs_new = evolve(coeffs_old, noise, decay, amplitude, waves)

    def per_slot(pair):
        coeff, basis = pair
        return jnp.einsum('rkej,lj->rel', coeff, basis, precision=lax.Precision.HIGHEST)
    field = lax.map(per_slot, (coeffs_new, legendre))
    real_part = jnp.zeros((M,) + field.shape[2:], field.dtype).at[waves].set(field[:, 0])
    imag_part = jnp.zeros((M,) + field.shape[2:], field.dtype).at[waves].set(field[:, 1])
    positive = jnp.arange(M, dtype=jnp.int32)[:, None, None] > 0
    imag_part = jnp.where(positive, imag_part, jnp.zeros_like(imag_part))
    real_part = jnp.take(real_part, lat_order.astype(jnp.int32), axis=2)
    imag_part = jnp.take(imag_part, lat_order.astype(jnp.int32), axis=2)
    spectrum = real_part + 1j * imag_part
    grid = jnp.fft.irfft(spectrum, n=LON, axis=0) * LON
    pattern = jnp.transpose(grid, (2, 1, 0))
    return (coeffs_new, pattern)
```

```python
import functools

import jax
import jax.numpy as jnp
from jax import lax
from jax.experimental import pallas as pl
from jax.experimental.pallas import tpu as pltpu
from jax.sharding import PartitionSpec as P

TWO_PI = 6.283185307179586
LANES = 128


def group_size(slots):
    return 4 if slots % 4 == 0 else slots


def split(x):
    high = x.astype(jnp.bfloat16)
    return high, (x - high.astype(jnp.float32)).astype(jnp.bfloat16)


def factors(decay, amplitude, waves):
    width = amplitude.shape[1]
    offsets = lax.broadcasted_iota(jnp.int32, (waves.shape[0], width), 1)
    live = (waves[:, None] + offsets < width).astype(jnp.float32)
    padded = jnp.concatenate([amplitude, jnp.zeros_like(amplitude)], axis=1)
    spread = jax.vmap(lambda wave: lax.dynamic_slice_in_dim(padded, wave, width, 1))(waves)
    fresh = spread * jnp.sqrt(1.0 - decay * decay)[None, :, None] * live[:, None, :]
    keep = decay[None, :, None] * live[:, None, :]
    return keep, fresh


def transform_kernel(order_ref, old_ref, noise_ref, basis_ref, keep_ref, fresh_ref, new_ref, send_ref, weights, field):
    group, step = pl.num_programs(1), pl.program_id(1)
    scales, members = old_ref.shape[2], old_ref.shape[3]
    devices, rows, wide = send_ref.shape[1:]
    lat_dev = order_ref.shape[0] // devices

    @pl.when((pl.program_id(0) == 0) & (step == 0))
    def _():
        weights[...] = jnp.zeros_like(weights)

    for part in range(2):
        total = None
        for scale in range(scales):
            keep = keep_ref[0, scale : scale + 1, :]
            fresh = fresh_ref[0, scale : scale + 1, :]
            value = keep * old_ref[0, part, scale] + fresh * noise_ref[0, part, scale].astype(jnp.float32)
            new_ref[0, part, scale] = value
            total = value if total is None else total + value
        weights[part * 64 : part * 64 + members, :] = total
    high, low = split(weights[...])
    both = jnp.concatenate([high, low], axis=0)
    basis_high, basis_low = split(basis_ref[0])
    contract = (((1,), (1,)), ((), ()))
    first = lax.dot_general(basis_high, both, contract, preferred_element_type=jnp.float32)
    second = lax.dot_general(basis_low, high, contract, preferred_element_type=jnp.float32)
    product = first[:, :LANES] + first[:, LANES:] + second
    other = pltpu.roll(product, 64, axis=1)
    for index in range(rows // 2):

        @pl.when(step == index)
        def _(index=index):
            field[:, 2 * index, :] = product
            field[:, 2 * index + 1, :] = other

    @pl.when(step == group - 1)
    def _():
        lane = lax.broadcasted_iota(jnp.int32, (rows, LANES), 1)

        def pack(device, carry):
            tiles = [jnp.zeros((rows, LANES), jnp.float32) for _ in range(wide // LANES)]
            for q in range(lat_dev):
                piece = field[order_ref[device * lat_dev + q]]
                start = members * q
                offset = start % LANES
                if offset:
                    piece = pltpu.roll(piece, offset, axis=1)
                tile = start // LANES
                tiles[tile] = jnp.where((lane >= offset) & (lane < offset + members), piece, tiles[tile])
                if offset + members > LANES:
                    tiles[tile + 1] = jnp.where(lane < offset + members - LANES, piece, tiles[tile + 1])
            for index, tile in enumerate(tiles):
                send_ref[0, device, :, index * LANES : (index + 1) * LANES] = tile
            return carry

        lax.fori_loop(0, devices, pack, 0)


def transform(coeffs_old, noise, legendre, keep, fresh, lat_order, devices):
    slots, parts, scales, members, width = coeffs_old.shape
    lats = legendre.shape[1]
    group = group_size(slots)
    rows = group * parts
    wide = -(-(lats // devices * members) // LANES) * LANES

    def slot5(g, i, order):
        return (g * group + i, 0, 0, 0, 0)

    def slot3(g, i, order):
        return (g * group + i, 0, 0)

    spec = pltpu.PrefetchScalarGridSpec(
        num_scalar_prefetch=1,
        grid=(slots // group, group),
        in_specs=[
            pl.BlockSpec((1, parts, scales, members, width), slot5),
            pl.BlockSpec((1, parts, scales, members, width), slot5),
            pl.BlockSpec((1, lats, width), slot3),
            pl.BlockSpec((1, scales, width), slot3),
            pl.BlockSpec((1, scales, width), slot3),
        ],
        out_specs=[
            pl.BlockSpec((1, parts, scales, members, width), slot5),
            pl.BlockSpec((1, devices, rows, wide), lambda g, i, order: (g, 0, 0, 0)),
        ],
        scratch_shapes=[
            pltpu.VMEM((LANES, width), jnp.float32),
            pltpu.VMEM((lats, rows, LANES), jnp.float32),
        ],
    )
    return pl.pallas_call(
        transform_kernel,
        grid_spec=spec,
        out_shape=[
            jax.ShapeDtypeStruct(coeffs_old.shape, jnp.float32),
            jax.ShapeDtypeStruct((slots // group, devices, rows, wide), jnp.float32),
        ],
        compiler_params=pltpu.CompilerParams(dimension_semantics=("arbitrary", "arbitrary")),
    )(lat_order, coeffs_old, noise, legendre, keep, fresh)


def synthesis_table(waves, length):
    column = lax.broadcasted_iota(jnp.int32, (waves.shape[0], length), 1)
    phase = waves[:, None] * column % length
    angle = phase.astype(jnp.float32) * (TWO_PI / length)
    weight = jnp.where(waves == 0, 1.0, 2.0).astype(jnp.float32)[:, None]
    return jnp.stack([weight * jnp.cos(angle), -weight * jnp.sin(angle)], axis=1).reshape(-1, length)


def local(coeffs_old, noise, legendre, decay, amplitude, wavenumber_of_slot, lat_order):
    devices = lax.axis_size("lat") * lax.axis_size("lon")
    me = lax.axis_index("lat") * lax.axis_size("lon") + lax.axis_index("lon")
    slots, parts, scales, members, width = coeffs_old.shape
    lats = legendre.shape[1]
    lons = 2 * lats
    lat_dev = lats // devices
    group = group_size(slots)
    mine = lax.dynamic_slice_in_dim(wavenumber_of_slot, me * slots, slots)
    keep, fresh = factors(decay, amplitude, mine)
    coeffs_new, send = transform(coeffs_old, noise, legendre, keep, fresh, lat_order, devices)
    got = lax.all_to_all(send, ("lat", "lon"), split_axis=1, concat_axis=1, tiled=True)
    ordered = wavenumber_of_slot.reshape(devices, slots // group, group).transpose(1, 0, 2).reshape(-1)
    table = synthesis_table(ordered, lons)
    values = got.reshape(-1, got.shape[-1])
    out = lax.dot_general(values, table, (((0,), (0,)), ((), ())), precision=lax.Precision.HIGH)
    pattern = out[: lat_dev * members].reshape(lat_dev, members, lons)
    return (coeffs_new, pattern)


def solution(mesh):
    split_rows = ("lat", "lon")
    in_specs = (
        P(split_rows, None, None, None, None),
        P(split_rows, None, None, None, None),
        P(split_rows, None, None),
        P(),
        P(),
        P(),
        P(),
    )
    out_specs = (P(split_rows, None, None, None, None), P(split_rows, None, None))
    return jax.shard_map(local, mesh=mesh, in_specs=in_specs, out_specs=out_specs, check_vma=False)
```
